32 devices in a mesh: boxes: 32 (over z, y, x, core).
Axes of the slice: x: 2, y: 2, z: 4, core: 2. Of those that a mesh axis runs over, the one named last changes fastest.
Arguments:
- conserved: float32 [32, 5, 16, 32, 128], P('boxes'), may hold values from -6 to 6
- volume_fraction: float32 [32, 16, 32, 128], P('boxes'), may hold values from 0.05 to 1
- cut_mask: int32 [32, 16, 32, 128], P('boxes'), may hold values 0 or 1
- merge_code: int32 [32, 16, 32, 128], P('boxes'), may hold values from 0 to 26
Outputs:
- redistributed: float32 [32, 5, 16, 32, 128], P('boxes')
The draws below stay inside these ranges and needn't reach their ends.
All inputs are finite; a program needn't handle non-finite values. No bound on the sum of `cut_mask` on one device may be relied on, other than what follows from the above.
Results may differ from the reference program's by a relative error of at most 0.0003.
Values sent between devices are 32-bit elements; how exact they have to be, the bound alone decides.
A program may use at most 64 MiB of HBM per device.

```python
import math
import jax
import jax.numpy as jnp
from jax import lax

FIELDS = 5
CX = 16
CY = 32
CZ = 128
NBY = 4
NBZ = 4
NBOXES = 32
NBX = 2
NX = 32
NY = 128
NZ = 512


def plant(array, stream_key, least, high):
    shape = array.shape
    spot = [jax.random.randint(jax.random.fold_in(stream_key, axis), (), 0, shape[axis]) for axis in range(len(shape))]
    array = array.at[tuple(spot)].set(least)
    longest = shape.index(max(shape))
    spot[longest] = (spot[longest] + 1) % shape[longest]
    return array.at[tuple(spot)].set(high)


def levels(key, dims, split, least, high):
    loudness, own = 1.0, jax.random.fold_in(key, 6)
    for dim, parts in split:
        steps = jnp.exp(jax.random.uniform(jax.random.fold_in(own, dim), (parts,), jnp.float32, least / len(split), high / len(split)))
        loudness = loudness * jnp.repeat(steps, dims[dim] // parts).reshape([-1 if axis == dim else 1 for axis in range(len(dims))])
    return loudness


def bell_draw(key, shape, width, limit, cuts=(), held_as=jnp.bfloat16):
    gain = levels(key, shape, cuts, -0.22, 0.18) if cuts else 1.0
    array = jax.random.normal(key, shape, jnp.float32) * width * gain
    return jnp.minimum(jnp.maximum(array, -limit), limit).astype(held_as)


def setup_inputs(seed: int = 0) -> dict:
    arg_keys = jax.random.split(jax.random.key(seed), 5)
    return {
        "conserved": bell_draw(arg_keys[0], (NBOXES, FIELDS, CX, CY, CZ), 1.0, 6.0, ((0, 32),), jnp.float32),
        "volume_fraction": jnp.clip(jnp.exp(math.log(1.0) - 2.9957323 * jax.random.uniform(arg_keys[1], (NBOXES, CX, CY, CZ), jnp.float32) ** levels(arg_keys[1], (NBOXES, CX, CY, CZ), ((0, 32),), -0.2, 0.2)), 0.05, 1.0),
        "cut_mask": plant((jax.random.randint(arg_keys[2], (NBOXES, CX, CY, CZ), 0, 2) < 1).astype(jnp.int32), jax.random.fold_in(arg_keys[2], 1), 0, 1),
        "merge_code": plant(jax.random.randint(arg_keys[3], (NBOXES, CX, CY, CZ), 0, 27), jax.random.fold_in(arg_keys[3], 1), 0, 26).astype(jnp.int32),
    }


OFFSETS = [(first, second, third) for first in (-1, 0, 1) for second in (-1, 0, 1) for third in (-1, 0, 1) if (first, second, third) != (0, 0, 0)]


def decode(code_field):
    sign_parts = (code_field // 9 - 1, (code_field // 3) % 3 - 1, code_field % 3 - 1)
    members = []
    for offset in OFFSETS:
        inside = jnp.ones(code_field.shape, jnp.bool_)
        for direction, component in zip(sign_parts, offset):
            if component != 0:
                inside = inside & (direction == component)
        members.append(inside)
    return members


def placed(values, offset):
    spread = [(0, 0)] * (values.ndim - 3) + [(1 + component, 1 - component) for component in offset]
    return jnp.pad(values, spread)


def count_members(members):
    running = placed(jnp.ones(members[0].shape, jnp.float32), (0, 0, 0))
    for offset, inside in zip(OFFSETS, members):
        running = running + placed(inside.astype(jnp.float32), offset)
    return running


def window(weighted, offset, interior):
    starts = [0] + [1 + component for component in offset]
    limits = [weighted.shape[0]] + [anchor + extent for anchor, extent in zip(starts[1:], interior)]
    return lax.slice(weighted, starts, limits)


def neighbour_average(weighted, members):
    interior = [extent - 2 for extent in weighted.shape[1:]]
    running = window(weighted, (0, 0, 0), interior)
    for offset, inside in zip(OFFSETS, members):
        running = running + jnp.where(inside[None], window(weighted, offset, interior), 0.0)
    return running[1:] / running[0:1]


def spread_back(average, members):
    running = placed(average, (0, 0, 0))
    for offset, inside in zip(OFFSETS, members):
        running = running + placed(jnp.where(inside[None], average, 0.0), offset)
    return running


def to_grid(boxed):
    channels = boxed.shape[1]
    shaped = boxed.reshape(NBX, NBY, NBZ, channels, CX, CY, CZ)
    return shaped.transpose(3, 0, 4, 1, 5, 2, 6).reshape(channels, NX, NY, NZ)


def from_grid(gridded):
    channels = gridded.shape[0]
    shaped = gridded.reshape(channels, NBX, CX, NBY, CY, NBZ, CZ)
    return shaped.transpose(1, 3, 5, 0, 2, 4, 6).reshape(NBOXES, channels, CX, CY, CZ)


def reference(conserved, volume_fraction, cut_mask, merge_code):
    fields = to_grid(conserved)
    fraction = to_grid(volume_fraction[:, None])[0]
    code_field = jnp.where(to_grid(cut_mask[:, None])[0] == 1, to_grid(merge_code[:, None])[0], 13)
    members = decode(code_field)
    counts = count_members(members)[1:-1, 1:-1, 1:-1]
    weight = fraction / counts
    weighted = jnp.concatenate([weight[None], weight[None] * fields], axis=0)
    weighted = jnp.pad(weighted, ((0, 0), (1, 1), (1, 1), (1, 1)))
    average = neighbour_average(weighted, members)
    gathered = spread_back(average, members)[:, 1:-1, 1:-1, 1:-1]
    return from_grid(gathered / counts[None])
```

```python
import functools

import jax
import jax.numpy as jnp
from jax import lax
from jax.experimental import pallas as pl
from jax.experimental.pallas import tpu as pltpu
from jax.sharding import PartitionSpec as P

NBY = 4
NBZ = 4
MESH = pl.DeviceIdType.MESH
XP, XM, YP, YM, ZP, ZM = 1, 2, 4, 8, 16, 32
ONE, UP, DOWN = 10, 14, 18
PX, PY = 3, 8


def flag(ax, ay, az):
    return (
        {1: XP, -1: XM, 0: 0}[ax] | {1: YP, -1: YM, 0: 0}[ay] | {1: ZP, -1: ZM, 0: 0}[az]
    )


def holds(e, bits):
    return (e & bits) == bits


def kernel(n, dims, u_ref, vf_ref, mask_ref, code_ref, out_ref, ext_e, ext_f, cnt, w0, wp, wm, avg,
           raw_m, raw_c, ys_e, ys_f, yr_e, yr_f, cr_e, cr_f, zs, zr, load_sem, send_sem, recv_sem):
    fields, cx, cy, cz = dims
    chans = fields + 1
    me = lax.axis_index("boxes")
    bx, by, bz = me // (NBY * NBZ), me // NBZ % NBY, me % NBZ
    axes = {
        "x": (NBY * NBZ, bx > 0, bx < n // (NBY * NBZ) - 1),
        "y": (NBZ, by > 0, by < NBY - 1),
        "z": (1, bz > 0, bz < NBZ - 1),
    }
    lane = lax.broadcasted_iota(jnp.int32, (8, cz), 1)
    nyb = (cy + 8) // 8

    loads = [
        pltpu.make_async_copy(mask_ref.at[0], raw_m, load_sem.at[0]),
        pltpu.make_async_copy(code_ref.at[0], raw_c, load_sem.at[1]),
        pltpu.make_async_copy(vf_ref.at[0], ext_f.at[0, PX:PX + cx, PY:PY + cy], load_sem.at[2]),
        pltpu.make_async_copy(u_ref.at[0], ext_f.at[1:chans, PX:PX + cx, PY:PY + cy], load_sem.at[3]),
    ]
    for copy in loads:
        copy.start()

    barrier = pltpu.get_barrier_semaphore()
    total = jnp.int32(0)
    for stride, low, high in axes.values():
        for has, there in ((low, me - stride), (high, me + stride)):
            @pl.when(has)
            def _():
                pl.semaphore_signal(barrier, inc=1, device_id=(there,), device_id_type=MESH)
            total = total + has.astype(jnp.int32)
    pl.semaphore_wait(barrier, total)

    def copies(axis, ident, up, down):
        stride = axes[axis][0]
        out = []
        for d, (pair, there) in enumerate(((up, me + stride), (down, me - stride))):
            out.append(pltpu.make_async_remote_copy(
                src_ref=pair[0], dst_ref=pair[1], send_sem=send_sem.at[2 * ident + d],
                recv_sem=recv_sem.at[2 * ident + d], device_id=(there,), device_id_type=MESH))
        return axis, out

    def start(c):
        axis, (up, down) = c
        _, low, high = axes[axis]
        pl.when(high)(lambda: up.start())
        pl.when(low)(lambda: down.start())

    def recv(c):
        axis, (up, down) = c
        _, low, high = axes[axis]
        pl.when(low)(lambda: up.wait_recv())
        pl.when(high)(lambda: down.wait_recv())

    def sent(c):
        axis, (up, down) = c
        _, low, high = axes[axis]
        pl.when(high)(lambda: up.wait_send())
        pl.when(low)(lambda: down.wait_send())

    def x_face(ident, ref, lead, depth):
        box = slice(PY, PY + cy)
        at = lambda a, b: ref.at[lead + (slice(a, b), box)]
        end = PX + cx
        return copies("x", ident, (at(end - depth, end), at(PX - depth, PX)),
                      (at(PX, PX + depth), at(end, end + depth)))

    x_e = x_face(0, ext_e, (), 3)
    x_vf = x_face(1, ext_f, (slice(0, 1),), 2)
    x_u = x_face(2, ext_f, (slice(1, chans),), 2)
    y_e = copies("y", 3, (ys_e.at[0], yr_e.at[0]), (ys_e.at[1], yr_e.at[1]))
    y_f = copies("y", 4, (ys_f.at[0], yr_f.at[0]), (ys_f.at[1], yr_f.at[1]))
    c_e = copies("x", 5, (yr_e.at[:, cx - 3:cx], cr_e.at[0]), (yr_e.at[:, 0:3], cr_e.at[1]))
    c_f = copies("x", 6, (yr_f.at[:, :, cx - 2:cx], cr_f.at[0]), (yr_f.at[:, :, 0:2], cr_f.at[1]))
    spans = ((0, 1), (1, 1 + chans), (1 + chans, 1 + chans + fields))
    z_c = [copies("z", 7 + i, (zs.at[0, a:b], zr.at[0, a:b]), (zs.at[1, a:b], zr.at[1, a:b]))
           for i, (a, b) in enumerate(spans)]
    everything = [x_e, x_vf, x_u, y_e, y_f, c_e, c_f] + z_c

    loads[0].wait()
    loads[1].wait()

    def encode(p, _):
        c = raw_c[p]
        cut = raw_m[p] == 1
        third = (c * 171) >> 9
        sz = c - 3 * third
        ninth = (third * 171) >> 9
        sy = third - 3 * ninth
        bit = lambda test, value: jnp.where(test, value, 0)
        e = (bit(ninth == 2, XP) + bit(ninth == 0, XM) + bit(sy == 2, YP) + bit(sy == 0, YM)
             + bit(sz == 2, ZP + (1 << UP)) + bit(sz == 0, ZM + (1 << DOWN)))
        ext_e[PX + p, PY:PY + cy, :] = jnp.where(cut, e, 0) + (1 << ONE)
        return 0

    lax.fori_loop(0, cx, encode, 0)
    start(x_e)
    ys_e[0] = ext_e[PX:PX + cx, PY + cy - 4:PY + cy, :]
    ys_e[1] = ext_e[PX:PX + cx, PY:PY + 4, :]
    start(y_e)
    loads[2].wait()
    start(x_vf)
    loads[3].wait()
    start(x_u)
    for c in range(chans):
        ys_f[0, c] = ext_f[c, PX:PX + cx, PY + cy - 2:PY + cy, :]
        ys_f[1, c] = ext_f[c, PX:PX + cx, PY:PY + 2, :]
    start(y_f)

    end = PX + cx
    _, low, high = axes["x"]
    for has, (e0, e1), (f0, f1) in ((low, (0, 3), (1, 3)), (high, (end, end + 3), (end, end + 2))):
        @pl.when(jnp.logical_not(has))
        def _():
            ext_e[e0:e1, :, :] = jnp.full((e1 - e0,) + ext_e.shape[1:], 1 << ONE, jnp.int32)
            for c in range(chans):
                ext_f[c, f0:f1, :, :] = jnp.zeros((f1 - f0,) + ext_f.shape[2:], jnp.float32)
    _, low, high = axes["y"]
    for side, has in enumerate((low, high)):
        @pl.when(jnp.logical_not(has))
        def _():
            yr_e[side] = jnp.full(yr_e.shape[1:], 1 << ONE, jnp.int32)
            yr_f[side] = jnp.zeros(yr_f.shape[1:], jnp.float32)
    _, low, high = axes["z"]
    for side, has in enumerate((low, high)):
        @pl.when(jnp.logical_not(has))
        def _():
            zr[side] = jnp.zeros(zr.shape[1:], jnp.float32)

    recv(y_e)
    start(c_e)
    ext_e[PX:PX + cx, PY - 4:PY, :] = yr_e[0]
    ext_e[PX:PX + cx, PY + cy:PY + cy + 4, :] = yr_e[1]
    recv(y_f)
    start(c_f)
    for c in range(chans):
        ext_f[c, PX:PX + cx, PY - 2:PY, :] = yr_f[0, c]
        ext_f[c, PX:PX + cx, PY + cy:PY + cy + 2, :] = yr_f[1, c]
    for c in (x_e, c_e, x_vf, x_u, c_f):
        recv(c)
    _, low, high = axes["x"]
    for side, has, e0, f0 in ((0, low, 0, 1), (1, high, end, end)):
        @pl.when(has)
        def _():
            for ys, er, fr in ((0, PY - 4, PY - 2), (1, PY + cy, PY + cy)):
                ext_e[e0:e0 + 3, er:er + 4, :] = cr_e[side, ys]
                for c in range(chans):
                    ext_f[c, f0:f0 + 2, fr:fr + 2, :] = cr_f[side, ys, c]

    def blocks(p0, p1, count, row0, body):
        def plane(p, _):
            def block(b, _):
                body(p, row0 + 8 * b, (p - p0) * count + b)
                return 0
            return lax.fori_loop(0, count, block, 0)
        lax.fori_loop(p0, p1, plane, 0)

    def rows(ref, lead, p, r):
        return ref[lead + (p, pl.ds(r, 8), slice(None))]

    def pack(slot, k, to_upper, to_lower):
        here = lane == k
        zs[0, slot] = jnp.where(here, pltpu.roll(to_upper, lax.rem(k + 1, cz), 1), zs[0, slot])
        zs[1, slot] = jnp.where(here, pltpu.roll(to_lower, k, 1), zs[1, slot])

    def from_lower(slot, k):
        return pltpu.roll(zr[0, slot], lax.rem(cz - k, cz), 1)

    def from_upper(slot, k):
        return pltpu.roll(zr[1, slot], cz - 1 - k, 1)

    pairs = [(ax, ay) for ax in (-1, 0, 1) for ay in (-1, 0, 1)]

    def count_body(p, r, k):
        acc = rows(ext_e, (), p, r)
        for ax, ay in pairs:
            if (ax, ay) != (0, 0):
                e = rows(ext_e, (), p - ax, r - ay)
                acc = acc + jnp.where(holds(e, flag(ax, ay, 0)), e, 0)
        up, down = (acc >> UP) & 15, (acc >> DOWN) & 15
        inner = ((acc >> ONE) & 15) + jnp.where(lane == 0, 0, pltpu.roll(up, 1, 1))
        inner = inner + jnp.where(lane == cz - 1, 0, pltpu.roll(down, cz - 1, 1))
        cnt[p, pl.ds(r, 8), :] = inner.astype(jnp.float32)
        pack(0, k, up.astype(jnp.float32), down.astype(jnp.float32))

    blocks(PX - 2, end + 2, nyb, PY - 4, count_body)
    start(z_c[0])
    recv(z_c[0])

    def weight_body(p, r, k):
        c = rows(cnt, (), p, r)
        c = c + jnp.where(lane == 0, from_lower(0, k), 0.0)
        c = c + jnp.where(lane == cz - 1, from_upper(0, k), 0.0)
        cnt[p, pl.ds(r, 8), :] = c
        w = rows(ext_f, (0,), p, r) / c
        for ch in range(chans):
            v = w if ch == 0 else w * rows(ext_f, (ch,), p, r)
            w0[ch, p, pl.ds(r, 8), :] = v
            pack(1 + ch, k, v, v)

    blocks(PX - 2, end + 2, nyb, PY - 4, weight_body)
    start(z_c[1])
    recv(z_c[1])

    def shift_body(p, r, k):
        for ch in range(chans):
            v = rows(w0, (ch,), p, r)
            wp[ch, p, pl.ds(r, 8), :] = jnp.where(
                lane == cz - 1, from_upper(1 + ch, k), pltpu.roll(v, cz - 1, 1))
            wm[ch, p, pl.ds(r, 8), :] = jnp.where(
                lane == 0, from_lower(1 + ch, k), pltpu.roll(v, 1, 1))

    blocks(PX - 2, end + 2, nyb, PY - 4, shift_body)

    def average_body(p, r, k):
        e = rows(ext_e, (), p, r)
        m = {b: holds(e, b) for b in (XP, XM, YP, YM, ZP, ZM)}

        def along_z(ch, q, s):
            side = jnp.where(m[ZP], rows(wp, (ch,), q, s), jnp.where(m[ZM], rows(wm, (ch,), q, s), 0.0))
            return rows(w0, (ch,), q, s) + side

        def along_y(ch, q):
            side = jnp.where(m[YP], along_z(ch, q, r + 1), jnp.where(m[YM], along_z(ch, q, r - 1), 0.0))
            return along_z(ch, q, r) + side

        def whole(ch):
            side = jnp.where(m[XP], along_y(ch, p + 1), jnp.where(m[XM], along_y(ch, p - 1), 0.0))
            return along_y(ch, p) + side

        inverse = 1.0 / whole(0)
        for ch in range(1, chans):
            avg[ch - 1, p, pl.ds(r, 8), :] = whole(ch) * inverse

    blocks(PX - 1, end + 1, nyb, PY - 4, average_body)

    def deposit_body(p, r, k):
        acc = [[None] * 3 for _ in range(fields)]
        for ax, ay in pairs:
            e = rows(ext_e, (), p - ax, r - ay)
            ms = [holds(e, flag(ax, ay, az)) for az in (0, 1, -1)]
            for f in range(fields):
                v = rows(avg, (f,), p - ax, r - ay)
                for i in range(3):
                    term = v if (ax, ay, i) == (0, 0, 0) else jnp.where(ms[i], v, 0.0)
                    acc[f][i] = term if acc[f][i] is None else acc[f][i] + term
        for f in range(fields):
            here, up, down = acc[f]
            here = here + jnp.where(lane == 0, 0.0, pltpu.roll(up, 1, 1))
            here = here + jnp.where(lane == cz - 1, 0.0, pltpu.roll(down, cz - 1, 1))
            out_ref[0, f, p - PX, pl.ds(r - PY, 8), :] = here
            pack(1 + chans + f, k, up, down)

    blocks(PX, end, cy // 8, PY, deposit_body)
    start(z_c[2])
    recv(z_c[2])

    def final_body(p, r, k):
        inverse = 1.0 / rows(cnt, (), p, r)
        for f in range(fields):
            v = out_ref[0, f, p - PX, pl.ds(r - PY, 8), :]
            v = v + jnp.where(lane == 0, from_lower(1 + chans + f, k), 0.0)
            v = v + jnp.where(lane == cz - 1, from_upper(1 + chans + f, k), 0.0)
            out_ref[0, f, p - PX, pl.ds(r - PY, 8), :] = v * inverse

    blocks(PX, end, cy // 8, PY, final_body)
    for c in everything:
        sent(c)


def per_device(n, conserved, volume_fraction, cut_mask, merge_code):
    fields, cx, cy, cz = conserved.shape[1:]
    chans = fields + 1
    ext = (cx + 6, cy + 16, cz)
    f32, i32 = jnp.float32, jnp.int32
    scratch = [
        pltpu.VMEM(ext, i32), pltpu.VMEM((chans,) + ext, f32), pltpu.VMEM(ext, f32),
        pltpu.VMEM((chans,) + ext, f32), pltpu.VMEM((chans,) + ext, f32), pltpu.VMEM((chans,) + ext, f32),
        pltpu.VMEM((fields,) + ext, f32),
        pltpu.VMEM((cx, cy, cz), i32), pltpu.VMEM((cx, cy, cz), i32),
        pltpu.VMEM((2, cx, 4, cz), i32), pltpu.VMEM((2, chans, cx, 2, cz), f32),
        pltpu.VMEM((2, cx, 4, cz), i32), pltpu.VMEM((2, chans, cx, 2, cz), f32),
        pltpu.VMEM((2, 2, 3, 4, cz), i32), pltpu.VMEM((2, 2, chans, 2, 2, cz), f32),
        pltpu.VMEM((2, 1 + chans + fields, 8, cz), f32), pltpu.VMEM((2, 1 + chans + fields, 8, cz), f32),
        pltpu.SemaphoreType.DMA((4,)), pltpu.SemaphoreType.DMA((20,)), pltpu.SemaphoreType.DMA((20,)),
    ]
    return pl.pallas_call(
        functools.partial(kernel, n, (fields, cx, cy, cz)),
        out_shape=jax.ShapeDtypeStruct(conserved.shape, f32),
        in_specs=[pl.BlockSpec(memory_space=pl.ANY)] * 4,
        out_specs=pl.BlockSpec(memory_space=pltpu.VMEM),
        scratch_shapes=scratch,
        compiler_params=pltpu.CompilerParams(
            collective_id=0, has_side_effects=True, vmem_limit_bytes=48 * 1024 * 1024),
        name="redistribute",
    )(conserved, volume_fraction, cut_mask, merge_code)


def solution(mesh):
    return jax.shard_map(
        functools.partial(per_device, mesh.shape["boxes"]),
        mesh=mesh,
        in_specs=(
            P("boxes", None, None, None, None),
            P("boxes", None, None, None),
            P("boxes", None, None, None),
            P("boxes", None, None, None),
        ),
        out_specs=P("boxes", None, None, None, None),
        check_vma=False,
    )
```

```python
import functools

import jax
import jax.numpy as jnp
from jax import lax
from jax.experimental import pallas as pl
from jax.experimental.pallas import tpu as pltpu
from jax.sharding import PartitionSpec as P

NBY = 4
NBZ = 4
MESH = pl.DeviceIdType.MESH
XP, XM, YP, YM, ZP, ZM = 1, 2, 4, 8, 16, 32
ONE, UP, DOWN = 10, 14, 18
PX, PY = 3, 8


def flag(ax, ay, az):
    return (
        {1: XP, -1: XM, 0: 0}[ax] | {1: YP, -1: YM, 0: 0}[ay] | {1: ZP, -1: ZM, 0: 0}[az]
    )


def holds(e, bits):
    return (e & bits) == bits


def kernel(n, dims, u_ref, vf_ref, mask_ref, code_ref, out_ref, ext_e, ext_f, cnt, w0, wp, wm, avg,
           raw_m, raw_c, ys_e, ys_f, yr_e, yr_f, cr_e, cr_f, zs, zr, load_sem, send_sem, recv_sem):
    fields, cx, cy, cz = dims
    chans = fields + 1
    me = lax.axis_index("boxes")
    bx, by, bz = me // (NBY * NBZ), me // NBZ % NBY, me % NBZ
    axes = {
        "x": (NBY * NBZ, bx > 0, bx < n // (NBY * NBZ) - 1),
        "y": (NBZ, by > 0, by < NBY - 1),
        "z": (1, bz > 0, bz < NBZ - 1),
    }
    lane = lax.broadcasted_iota(jnp.int32, (8, cz), 1)
    nyb = (cy + 8) // 8

    loads = [
        pltpu.make_async_copy(mask_ref.at[0], raw_m, load_sem.at[0]),
        pltpu.make_async_copy(code_ref.at[0], raw_c, load_sem.at[1]),
        pltpu.make_async_copy(vf_ref.at[0], ext_f.at[0, PX:PX + cx, PY:PY + cy], load_sem.at[2]),
        pltpu.make_async_copy(u_ref.at[0], ext_f.at[1:chans, PX:PX + cx, PY:PY + cy], load_sem.at[3]),
    ]
    for copy in loads:
        copy.start()

    barrier = pltpu.get_barrier_semaphore()
    total = jnp.int32(0)
    for stride, low, high in axes.values():
        for has, there in ((low, me - stride), (high, me + stride)):
            @pl.when(has)
            def _():
                pl.semaphore_signal(barrier, inc=1, device_id=(there,), device_id_type=MESH)
            total = total + has.astype(jnp.int32)
    pl.semaphore_wait(barrier, total)

    def copies(axis, ident, up, down):
        stride = axes[axis][0]
        out = []
        for d, (pair, there) in enumerate(((up, me + stride), (down, me - stride))):
            out.append(pltpu.make_async_remote_copy(
                src_ref=pair[0], dst_ref=pair[1], send_sem=send_sem.at[2 * ident + d],
                recv_sem=recv_sem.at[2 * ident + d], device_id=(there,), device_id_type=MESH))
        return axis, out

    def start(c):
        axis, (up, down) = c
        _, low, high = axes[axis]
        pl.when(high)(lambda: up.start())
        pl.when(low)(lambda: down.start())

    def recv(c):
        axis, (up, down) = c
        _, low, high = axes[axis]
        pl.when(low)(lambda: up.wait_recv())
        pl.when(high)(lambda: down.wait_recv())

    def sent(c):
        axis, (up, down) = c
        _, low, high = axes[axis]
        pl.when(high)(lambda: up.wait_send())
        pl.when(low)(lambda: down.wait_send())

    def x_face(ident, ref, lead, depth):
        box = slice(PY, PY + cy)
        at = lambda a, b: ref.at[lead + (slice(a, b), box)]
        end = PX + cx
        return copies("x", ident, (at(end - depth, end), at(PX - depth, PX)),
                      (at(PX, PX + depth), at(end, end + depth)))

    x_e = x_face(0, ext_e, (), 3)
    x_vf = x_face(1, ext_f, (slice(0, 1),), 2)
    x_u = x_face(2, ext_f, (slice(1, chans),), 2)
    y_e = copies("y", 3, (ys_e.at[0], yr_e.at[0]), (ys_e.at[1], yr_e.at[1]))
    y_f = copies("y", 4, (ys_f.at[0], yr_f.at[0]), (ys_f.at[1], yr_f.at[1]))
    c_e = copies("x", 5, (yr_e.at[:, cx - 3:cx], cr_e.at[0]), (yr_e.at[:, 0:3], cr_e.at[1]))
    c_f = copies("x", 6, (yr_f.at[:, :, cx - 2:cx], cr_f.at[0]), (yr_f.at[:, :, 0:2], cr_f.at[1]))
    last = 1 + 2 * chans
    spans = ((0, 1), (1, 1 + chans), (1 + chans, last), (last, last + fields))
    z_c = [copies("z", 7 + i, (zs.at[0, a:b], zr.at[0, a:b]), (zs.at[1, a:b], zr.at[1, a:b]))
           for i, (a, b) in enumerate(spans)]
    everything = [x_e, x_vf, x_u, y_e, y_f, c_e, c_f] + z_c

    loads[0].wait()
    loads[1].wait()

    def encode(p, _):
        c = raw_c[p]
        cut = raw_m[p] == 1
        third = (c * 171) >> 9
        sz = c - 3 * third
        ninth = (third * 171) >> 9
        sy = third - 3 * ninth
        bit = lambda test, value: jnp.where(test, value, 0)
        e = (bit(ninth == 2, XP) + bit(ninth == 0, XM) + bit(sy == 2, YP) + bit(sy == 0, YM)
             + bit(sz == 2, ZP + (1 << UP)) + bit(sz == 0, ZM + (1 << DOWN)))
        ext_e[PX + p, PY:PY + cy, :] = jnp.where(cut, e, 0) + (1 << ONE)
        return 0

    lax.fori_loop(0, cx, encode, 0)
    start(x_e)
    ys_e[0] = ext_e[PX:PX + cx, PY + cy - 4:PY + cy, :]
    ys_e[1] = ext_e[PX:PX + cx, PY:PY + 4, :]
    start(y_e)
    loads[2].wait()
    start(x_vf)
    loads[3].wait()
    start(x_u)
    for c in range(chans):
        ys_f[0, c] = ext_f[c, PX:PX + cx, PY + cy - 2:PY + cy, :]
        ys_f[1, c] = ext_f[c, PX:PX + cx, PY:PY + 2, :]
    start(y_f)

    end = PX + cx
    _, low, high = axes["x"]
    for has, (e0, e1), (f0, f1) in ((low, (0, 3), (1, 3)), (high, (end, end + 3), (end, end + 2))):
        @pl.when(jnp.logical_not(has))
        def _():
            ext_e[e0:e1, :, :] = jnp.full((e1 - e0,) + ext_e.shape[1:], 1 << ONE, jnp.int32)
            for c in range(chans):
                ext_f[c, f0:f1, :, :] = jnp.zeros((f1 - f0,) + ext_f.shape[2:], jnp.float32)
    _, low, high = axes["y"]
    for side, has in enumerate((low, high)):
        @pl.when(jnp.logical_not(has))
        def _():
            yr_e[side] = jnp.full(yr_e.shape[1:], 1 << ONE, jnp.int32)
            yr_f[side] = jnp.zeros(yr_f.shape[1:], jnp.float32)
    _, low, high = axes["z"]
    for side, has in enumerate((low, high)):
        @pl.when(jnp.logical_not(has))
        def _():
            zr[side] = jnp.zeros(zr.shape[1:], jnp.float32)

    recv(y_e)
    start(c_e)
    ext_e[PX:PX + cx, PY - 4:PY, :] = yr_e[0]
    ext_e[PX:PX + cx, PY + cy:PY + cy + 4, :] = yr_e[1]
    recv(y_f)
    start(c_f)
    for c in range(chans):
        ext_f[c, PX:PX + cx, PY - 2:PY, :] = yr_f[0, c]
        ext_f[c, PX:PX + cx, PY + cy:PY + cy + 2, :] = yr_f[1, c]
    recv(x_e)
    recv(c_e)
    x_sides = [(side, has, at) for side, (has, at) in enumerate(zip(axes["x"][1:], (PX, end)))]
    for side, has, at in x_sides:
        @pl.when(has)
        def _():
            e0 = at - 3 if side == 0 else at
            for ys, er in ((0, PY - 4), (1, PY + cy)):
                ext_e[e0:e0 + 3, er:er + 4, :] = cr_e[side, ys]

    zero = me // n

    def blocks(planes, p0, count, row0, body):
        steps, plane_of = planes
        group = count

        def several(p, b0, size):
            packs = []
            for i in range(size):
                b = b0 + i
                k = (p - p0) * count + b
                packs.append((k, body(p, row0 + zero + 8 * b, k)))
            for j in range(len(packs[0][1])):
                slot = packs[0][1][j][0]
                upper, lower = zs[0, slot], zs[1, slot]
                for k, found in packs:
                    _, to_upper, to_lower = found[j]
                    here = lane == k
                    upper = jnp.where(here, pltpu.roll(to_upper, lax.rem(k + 1, cz), 1), upper)
                    lower = jnp.where(here, pltpu.roll(to_lower, k, 1), lower)
                zs[0, slot] = upper
                zs[1, slot] = lower

        def plane(i, _):
            several(plane_of(i), 0, count)
            return 0

        lax.fori_loop(0, steps, plane, 0)

    def span(p0, p1):
        return p1 - p0, lambda i: i + p0

    def both_ends(p0, p1):
        return 4, lambda i: i + p0 + i // 2 * (p1 - p0 - 4)

    def rows(ref, lead, p, r):
        return ref[lead + (p, pl.ds(r, 8), slice(None))]

    def from_lower(slot, k):
        return pltpu.roll(zr[0, slot], lax.rem(cz - k, cz), 1)

    def from_upper(slot, k):
        return pltpu.roll(zr[1, slot], cz - 1 - k, 1)

    pairs = [(ax, ay) for ax in (-1, 0, 1) for ay in (-1, 0, 1)]

    def count_body(p, r, k):
        acc = rows(ext_e, (), p, r)
        for ax, ay in pairs:
            if (ax, ay) != (0, 0):
                e = rows(ext_e, (), p - ax, r - ay)
                acc = acc + jnp.where(holds(e, flag(ax, ay, 0)), e, 0)
        up, down = (acc >> UP) & 15, (acc >> DOWN) & 15
        inner = ((acc >> ONE) & 15) + jnp.where(lane == 0, 0, pltpu.roll(up, 1, 1))
        inner = inner + jnp.where(lane == cz - 1, 0, pltpu.roll(down, cz - 1, 1))
        cnt[p, pl.ds(r, 8), :] = inner.astype(jnp.float32)
        return [(0, up.astype(jnp.float32), down.astype(jnp.float32))]

    blocks(span(PX - 2, end + 2), PX - 2, nyb, PY - 4, count_body)
    start(z_c[0])
    recv(z_c[0])

    def weight_body(slot, p, r, k):
        c = rows(cnt, (), p, r)
        c = c + jnp.where(lane == 0, from_lower(0, k), 0.0)
        c = c + jnp.where(lane == cz - 1, from_upper(0, k), 0.0)
        cnt[p, pl.ds(r, 8), :] = c
        w = rows(ext_f, (0,), p, r) / c
        packs = []
        for ch in range(chans):
            v = w if ch == 0 else w * rows(ext_f, (ch,), p, r)
            w0[ch, p, pl.ds(r, 8), :] = v
            packs.append((slot + ch, v, v))
        return packs

    def shift_body(slot, p, r, k):
        for ch in range(chans):
            v = rows(w0, (ch,), p, r)
            wp[ch, p, pl.ds(r, 8), :] = jnp.where(
                lane == cz - 1, from_upper(slot + ch, k), pltpu.roll(v, cz - 1, 1))
            wm[ch, p, pl.ds(r, 8), :] = jnp.where(
                lane == 0, from_lower(slot + ch, k), pltpu.roll(v, 1, 1))
        return []

    def average_body(p, r, k):
        e = rows(ext_e, (), p, r)
        m = {b: holds(e, b) for b in (XP, XM, YP, YM, ZP, ZM)}

        def along_z(ch, q, s):
            side = jnp.where(m[ZP], rows(wp, (ch,), q, s), jnp.where(m[ZM], rows(wm, (ch,), q, s), 0.0))
            return rows(w0, (ch,), q, s) + side

        def along_y(ch, q):
            side = jnp.where(m[YP], along_z(ch, q, r + 1), jnp.where(m[YM], along_z(ch, q, r - 1), 0.0))
            return along_z(ch, q, r) + side

        def whole(ch):
            side = jnp.where(m[XP], along_y(ch, p + 1), jnp.where(m[XM], along_y(ch, p - 1), 0.0))
            return along_y(ch, p) + side

        inverse = 1.0 / whole(0)
        for ch in range(1, chans):
            avg[ch - 1, p, pl.ds(r, 8), :] = whole(ch) * inverse
        return []

    def deposit_body(p, r, k):
        acc = [[None] * 3 for _ in range(fields)]
        for ax, ay in pairs:
            e = rows(ext_e, (), p - ax, r - ay)
            ms = [holds(e, flag(ax, ay, az)) for az in (0, 1, -1)]
            for f in range(fields):
                v = rows(avg, (f,), p - ax, r - ay)
                for i in range(3):
                    term = v if (ax, ay, i) == (0, 0, 0) else jnp.where(ms[i], v, 0.0)
                    acc[f][i] = term if acc[f][i] is None else acc[f][i] + term
        packs = []
        for f in range(fields):
            here, up, down = acc[f]
            here = here + jnp.where(lane == 0, 0.0, pltpu.roll(up, 1, 1))
            here = here + jnp.where(lane == cz - 1, 0.0, pltpu.roll(down, cz - 1, 1))
            out_ref[0, f, p - PX, pl.ds(r - PY, 8), :] = here
            packs.append((1 + 2 * chans + f, up, down))
        return packs

    weight = lambda planes, slot: blocks(
        planes, PX - 2, nyb, PY - 4, functools.partial(weight_body, slot))
    shift = lambda planes, slot: blocks(
        planes, PX - 2, nyb, PY - 4, functools.partial(shift_body, slot))
    average = lambda planes: blocks(planes, PX - 1, nyb, PY - 4, average_body)
    deposit = lambda planes: blocks(planes, PX, cy // 8, PY, deposit_body)

    own, ghosts = span(PX, end), both_ends(PX - 2, end + 2)
    weight(own, 1)
    start(z_c[1])
    recv(z_c[1])
    shift(own, 1)
    average(span(PX + 1, end - 1))
    for c in (x_vf, x_u, c_f):
        recv(c)
    for side, has, at in x_sides:
        @pl.when(has)
        def _():
            f0 = at - 2 if side == 0 else at
            for ys, fr in ((0, PY - 2), (1, PY + cy)):
                for c in range(chans):
                    ext_f[c, f0:f0 + 2, fr:fr + 2, :] = cr_f[side, ys, c]
    weight(ghosts, 1 + chans)
    start(z_c[2])
    deposit(span(PX + 2, end - 2))
    recv(z_c[2])
    shift(ghosts, 1 + chans)
    average(both_ends(PX - 1, end + 1))
    deposit(both_ends(PX, end))
    start(z_c[3])
    recv(z_c[3])

    def final_body(p, r, k):
        inverse = 1.0 / rows(cnt, (), p, r)
        for f in range(fields):
            v = out_ref[0, f, p - PX, pl.ds(r - PY, 8), :]
            v = v + jnp.where(lane == 0, from_lower(1 + 2 * chans + f, k), 0.0)
            v = v + jnp.where(lane == cz - 1, from_upper(1 + 2 * chans + f, k), 0.0)
            out_ref[0, f, p - PX, pl.ds(r - PY, 8), :] = v * inverse
        return []

    blocks(own, PX, cy // 8, PY, final_body)
    for c in everything:
        sent(c)


def per_device(n, conserved, volume_fraction, cut_mask, merge_code):
    fields, cx, cy, cz = conserved.shape[1:]
    chans = fields + 1
    ext = (cx + 7, cy + 24, cz)
    f32, i32 = jnp.float32, jnp.int32
    scratch = [
        pltpu.VMEM(ext, i32), pltpu.VMEM((chans,) + ext, f32), pltpu.VMEM(ext, f32),
        pltpu.VMEM((chans,) + ext, f32), pltpu.VMEM((chans,) + ext, f32), pltpu.VMEM((chans,) + ext, f32),
        pltpu.VMEM((fields,) + ext, f32),
        pltpu.VMEM((cx, cy, cz), i32), pltpu.VMEM((cx, cy, cz), i32),
        pltpu.VMEM((2, cx, 4, cz), i32), pltpu.VMEM((2, chans, cx, 2, cz), f32),
        pltpu.VMEM((2, cx, 4, cz), i32), pltpu.VMEM((2, chans, cx, 2, cz), f32),
        pltpu.VMEM((2, 2, 3, 4, cz), i32), pltpu.VMEM((2, 2, chans, 2, 2, cz), f32),
        pltpu.VMEM((2, 1 + 2 * chans + fields, 8, cz), f32), pltpu.VMEM((2, 1 + 2 * chans + fields, 8, cz), f32),
        pltpu.SemaphoreType.DMA((4,)), pltpu.SemaphoreType.DMA((22,)), pltpu.SemaphoreType.DMA((22,)),
    ]
    return pl.pallas_call(
        functools.partial(kernel, n, (fields, cx, cy, cz)),
        out_shape=jax.ShapeDtypeStruct(conserved.shape, f32),
        in_specs=[pl.BlockSpec(memory_space=pl.ANY)] * 4,
        out_specs=pl.BlockSpec(memory_space=pltpu.VMEM),
        scratch_shapes=scratch,
        compiler_params=pltpu.CompilerParams(
            collective_id=0, has_side_effects=True, vmem_limit_bytes=60 * 1024 * 1024),
        name="redistribute",
    )(conserved, volume_fraction, cut_mask, merge_code)


def solution(mesh):
    return jax.shard_map(
        functools.partial(per_device, mesh.shape["boxes"]),
        mesh=mesh,
        in_specs=(
            P("boxes", None, None, None, None),
            P("boxes", None, None, None),
            P("boxes", None, None, None),
            P("boxes", None, None, None),
        ),
        out_specs=P("boxes", None, None, None, None),
        check_vma=False,
    )
```
